512 devices in a mesh: gz: 8 (over y, core), row: 16 (over z), col: 4 (over x).
Axes of the slice: x: 4, y: 4, z: 16, core: 2. Of those that a mesh axis runs over, the one named last changes fastest.
Arguments:
- lpanel: bfloat16 [2, 8, 4096, 2048], P(None, 'gz', 'row', 'col'), may hold values from -6 to 6
- upanel: bfloat16 [2, 8, 2048, 4096], P(None, 'gz', 'row', 'col'), may hold values from -0.125 to 0.125
- rowmap: int32 [2, 8, 16], P(None, 'gz', 'row'), may hold values from 0 to 1
- colmap: int32 [2, 8, 16], P(None, 'gz', 'col'), may hold values from 0 to 7
- blockmask: int32 [2, 8, 16, 16], P(None, 'gz', 'row', 'col'), may hold values 0 or 1
- front_blocks: bfloat16 [2, 8192, 8192], P(None, 'row', ('gz', 'col')), may hold values from -6 to 6
Outputs:
- front_update: bfloat16 [2, 8192, 8192], P(None, 'row', ('gz', 'col'))
The draws below stay inside these ranges and needn't reach their ends.
All inputs are finite; a program needn't handle non-finite values. No bound on the sum of `blockmask` on one device may be relied on, other than what follows from the above.
Results may differ from the reference program's by a relative error of at most 0.008.
Values may be sent and summed in bfloat16 or wider, within the bound.
A program may use at most 64 MiB of HBM per device.

```python
import math
import jax
import jax.numpy as jnp
import numpy as np
from jax import lax

B = 256
W = 2048
CB = 4
FRB = 2
LEVELS = 2
UR = 4096
UC = 4096
FR = 8192
FC = 8192
N_GZ = 8
N_ROW = 16
N_COL = 4


def set_ends(values, rng, low, top_value):
    extent = values.shape
    place = [jax.random.randint(jax.random.fold_in(rng, axis), (), 0, extent[axis]) for axis in range(len(extent))]
    values = values.at[tuple(place)].set(low)
    longest = extent.index(max(extent))
    place[longest] = (place[longest] + 1) % extent[longest]
    return values.at[tuple(place)].set(top_value)


def level_of(rng, extent, cuts, least, top_value):
    gain = 1.0
    for position, blocks in cuts:
        draws = jax.random.uniform(jax.random.fold_in(jax.random.fold_in(rng, 6), position), (blocks,), jnp.float32, least / len(cuts), top_value / len(cuts))
        gain = gain * jnp.repeat(jnp.exp(draws), extent[position] // blocks).reshape((-1,) + (1,) * (len(extent) - 1 - position))
    return gain


def rank_bounds(amount, slope):
    portions = [(1 << 20) // math.isqrt(standing ** slope) + 1 for standing in range(1, amount + 1)]
    spread = 1 + sum(portions) // (1 << 30)
    return np.cumsum(np.array([max(1, weight // spread) for weight in portions]))


def ranked(own_key, extent, amount, slope):
    table = rank_bounds(amount, slope)
    pick = jax.random.randint(jax.random.fold_in(own_key, 1), extent, 0, int(table[amount - 1]))
    rank = jnp.searchsorted(jnp.asarray(table, jnp.int32), pick, side="right")
    return jax.random.permutation(jax.random.fold_in(own_key, 2), amount)[rank].astype(jnp.int32)


def gaussian(rng, shape, width, limit, pieces=(), kind=jnp.bfloat16):
    values = jax.random.normal(rng, shape, jnp.float32) * width
    if len(pieces) > 0:
        values = level_of(rng, shape, pieces, -0.22, 0.18) * values
    return jnp.clip(values, min=-limit, max=limit).astype(kind)


def setup_inputs(seed: int = 0) -> dict:
    key_list = jax.random.split(jax.random.key(seed), 7)
    lpanel = gaussian(key_list[0], (LEVELS, N_GZ, UR, W), 1.0, 6.0, ((1, 8), (2, 16), (3, 4)))
    upanel = gaussian(key_list[1], (LEVELS, N_GZ, W, UC), W ** -0.5, 0.125, ((1, 8), (2, 16), (3, 4)))
    rowmap = set_ends(jax.random.randint(key_list[2], (LEVELS, N_GZ, N_ROW), 0, FRB), jax.random.fold_in(key_list[2], 1), 0, FRB - 1).astype(jnp.int32)
    colmap = set_ends(ranked(key_list[3], (LEVELS, N_GZ, N_COL * CB), N_GZ, 2), jax.random.fold_in(key_list[3], 3), 0, N_GZ - 1).astype(jnp.int32)
    blockmask = set_ends((jax.random.randint(key_list[4], (LEVELS, N_GZ, N_ROW, N_COL * CB), 0, 4) < 3).astype(jnp.int32), jax.random.fold_in(key_list[4], 1), 0, 1)
    front_blocks = gaussian(key_list[5], (LEVELS, FR, FC), 1.0, 6.0, ((1, 16), (2, 32)))
    return dict(lpanel=lpanel, upanel=upanel, rowmap=rowmap, colmap=colmap, blockmask=blockmask, front_blocks=front_blocks)


def layer_partial(schur, rows_of, cols_of, live):
    blocks = schur.reshape(N_ROW, B, N_COL, CB, B)
    targets = cols_of.reshape(N_COL, CB)[:, :, None] == jnp.arange(N_GZ, dtype=jnp.int32)[None, None, :]
    col_select = targets.astype(jnp.float32)[None] * live.reshape(N_ROW, N_COL, CB).astype(jnp.float32)[:, :, :, None]
    col_sums = jnp.einsum("rbcjk,rcjl->rblck", blocks, col_select, precision=lax.Precision.HIGHEST)
    row_select = (rows_of[:, None] == jnp.arange(FRB, dtype=jnp.int32)[None, :]).astype(jnp.float32)
    placed = row_select[:, :, None, None, None, None] * col_sums[:, None]
    return placed.reshape(FR, FC)


def reference(lpanel, upanel, rowmap, colmap, blockmask, front_blocks):
    results = []
    for depth in range(LEVELS):
        total = jnp.zeros((FR, FC), jnp.float32)
        for layer in range(N_GZ):
            schur = jnp.dot(lpanel[depth, layer], upanel[depth, layer], preferred_element_type=jnp.float32)
            partial_value = layer_partial(schur, rowmap[depth, layer], colmap[depth, layer], blockmask[depth, layer])
            total = total + partial_value.astype(jnp.bfloat16).astype(jnp.float32)
        results.append((front_blocks[depth].astype(jnp.float32) - total).astype(jnp.bfloat16))
    return jnp.stack(results)
```

```python
import functools

import jax
import jax.numpy as jnp
from jax import lax
from jax.experimental import pallas as pl
from jax.experimental.pallas import tpu as pltpu
from jax.sharding import PartitionSpec as P

MESH = pl.DeviceIdType.MESH
CB = 4
FRB = 2
LEVELS = 2
HALVES = 2
SUBS = 4


def kernel(
    n_row, n_gz, n_col,
    l_hbm, u_hbm, rowmap_hbm, colmap_hbm, mask_hbm, front_hbm,
    out_hbm,
    u_all, l_all, acc, sums, arrived, rows_of, front, result,
    rowmap, colmap, mask,
    zsend, zrecv, lsend, lrecv, asend, arecv, rsend, rrecv, usem, lsem, fsem, osem, isem,
):
    row, gz, col = lax.axis_index("row"), lax.axis_index("gz"), lax.axis_index("col")
    phases = LEVELS * HALVES
    depth = u_hbm.shape[2]
    width = l_hbm.shape[2]
    half = width // HALVES
    lblocks = l_hbm.shape[3] // depth
    last = n_row // 2 - 1
    piece = depth // SUBS
    ring = [lax.rem(row + 1, n_row), lax.rem(row + n_row - 1, n_row)]

    def others(me, n):
        return [lax.rem(me + i, n) for i in range(1, n)]

    cores = 2
    chips = n_gz // cores
    chip, core = lax.div(gz, cores), lax.rem(gz, cores)
    order = sorted(range(1, chips), key=lambda d: -min(d, chips - d)) + [0]
    peers = []
    for d in order:
        for k in range(cores):
            if (d, k) != (0, 0):
                peers.append(lax.rem(chip + d, chips) * cores + lax.rem(core + k, cores))

    def own_u(p, j):
        v, h = divmod(p, HALVES)
        return pltpu.make_async_copy(
            u_hbm.at[v, 0, :, pl.ds(j * width + h * half, half)],
            u_all.at[p, pl.ds(row * depth, depth), pl.ds(j * half, half)],
            usem.at[p, j],
        )

    def own_l(v, i):
        return pltpu.make_async_copy(
            l_hbm.at[v, 0, :, pl.ds(i * depth, depth)], l_all.at[v, col * lblocks + i], lsem.at[v, i]
        )

    fronts = pltpu.make_async_copy(front_hbm, front, fsem)
    maps = [
        pltpu.make_async_copy(rowmap_hbm, rowmap, isem.at[0]),
        pltpu.make_async_copy(colmap_hbm, colmap, isem.at[1]),
        pltpu.make_async_copy(mask_hbm, mask, isem.at[2]),
    ]
    for j in range(CB):
        own_u(0, j).start()
    for i in range(lblocks):
        own_l(0, i).start()
    for p in range(1, phases):
        for j in range(CB):
            own_u(p, j).start()
    for v in range(1, LEVELS):
        for i in range(lblocks):
            own_l(v, i).start()
    fronts.start()
    for copy in maps:
        copy.start()

    barrier = pltpu.get_barrier_semaphore()
    for r in ring:
        pl.semaphore_signal(barrier, inc=1, device_id={"row": r}, device_id_type=MESH)
    for c in others(col, n_col):
        pl.semaphore_signal(barrier, inc=1, device_id={"col": c}, device_id_type=MESH)
    for g in peers:
        pl.semaphore_signal(barrier, inc=1, device_id={"gz": g}, device_id_type=MESH)
    pl.semaphore_wait(barrier, 2 + (n_col - 1) + (n_gz - 1))

    def hop(way, p, t, s):
        shard = lax.rem(row + n_row - t, n_row) if way == 0 else lax.rem(row + t, n_row)
        at = u_all.at[p, pl.ds(pl.multiple_of(shard * depth + s * piece, piece), piece)]
        return pltpu.make_async_remote_copy(
            src_ref=at, dst_ref=at, send_sem=zsend.at[way, p], recv_sem=zrecv.at[way, p, t, s],
            device_id={"row": ring[way]}, device_id_type=MESH,
        )

    def arrival(way, p, t, s):
        at = u_all.at[p, pl.ds(0, piece)]
        return pltpu.make_async_copy(at, at, zrecv.at[way, p, t, s])

    longer = (range(SUBS // 2), range(SUBS // 2, SUBS))

    def send_own(p):
        for j in range(CB):
            own_u(p, j).wait()
        for s in range(SUBS):
            for way in range(2):
                hop(way, p, 0, (s + way * SUBS // 2) % SUBS).start()

    def forward(p, t):
        for s in range(SUBS):
            for way in range(2):
                which = (s + way * SUBS // 2) % SUBS
                arrival(way, p, t - 1, which).wait()
                hop(way, p, t, which).start()

    def forward_last(p):
        for s in range(SUBS):
            for way in range(2):
                which = (s + way * SUBS // 2) % SUBS
                arrival(way, p, last - 1, which).wait()
                if which in longer[way]:
                    hop(way, p, last, which).start()

    def wait_last(p):
        for way in range(2):
            for s in longer[way]:
                arrival(way, p, last, s).wait()

    def l_copy(v, c):
        at = l_all.at[v, pl.ds(col * lblocks, lblocks)]
        return pltpu.make_async_remote_copy(
            src_ref=at, dst_ref=at, send_sem=lsend, recv_sem=lrecv.at[v, col],
            device_id={"col": c}, device_id_type=MESH,
        )

    def send_l(v):
        for i in range(lblocks):
            own_l(v, i).wait()
        for c in others(col, n_col):
            l_copy(v, c).start()

    def wait_l(v):
        at = l_all.at[v, pl.ds(0, lblocks)]
        for c in others(col, n_col):
            pltpu.make_async_copy(at, at, lrecv.at[v, c]).wait()

    def rows_copy(g):
        at = rows_of.at[gz]
        return pltpu.make_async_remote_copy(
            src_ref=at, dst_ref=at, send_sem=rsend, recv_sem=rrecv.at[gz],
            device_id={"gz": g}, device_id_type=MESH,
        )

    def wait_rows():
        at = rows_of.at[0]
        for g in peers:
            pltpu.make_async_copy(at, at, rrecv.at[g]).wait()

    def product(p, first, count):
        v = p // HALVES
        left = jnp.concatenate([l_all[v, first + i] for i in range(count)], axis=1) if count > 1 else l_all[v, first]
        right = u_all[p, pl.ds(pl.multiple_of(first * depth, depth), count * depth), :]
        return jnp.dot(left, right, preferred_element_type=jnp.float32)

    def products(p, q, parts):
        size = n_row // parts
        value = product(p, q * size, size)
        if q == 0:
            acc[p % 2] = value
        else:
            acc[p % 2] += value

    def block_copy(p, g):
        return pltpu.make_async_remote_copy(
            src_ref=sums.at[p, g], dst_ref=arrived.at[p, gz], send_sem=asend.at[p], recv_sem=arecv.at[p, gz],
            device_id={"gz": g}, device_id_type=MESH,
        )

    def layer_sum(p, g):
        v = p // HALVES
        total = None
        for j in range(CB):
            keep = jnp.where(colmap[v, 0, j] == g, mask[v, 0, 0, j], 0).astype(jnp.float32)
            term = acc[p % 2, :, j * half : (j + 1) * half] * keep
            total = term if total is None else total + term
        return total.astype(jnp.bfloat16)

    def exchange(p):
        before = None
        for g in peers:
            sums[p, g] = layer_sum(p, g)
            if before is not None:
                block_copy(p, before).start()
            before = g
        arrived[p, gz] = layer_sum(p, gz)
        block_copy(p, before).start()

    def out_copy(p):
        v, h = divmod(p, HALVES)
        at = (v, slice(None), pl.ds(h * half, half))
        return pltpu.make_async_copy(result.at[at], out_hbm.at[at], osem.at[p])

    def finish(p):
        v, h = divmod(p, HALVES)
        block = arrived.at[p, 0]
        for g in peers:
            pltpu.make_async_copy(block, block, arecv.at[p, g]).wait()
        placed = [None] * FRB
        for g in range(n_gz):
            value = arrived[p, g].astype(jnp.float32)
            target = rows_of[g, v][:1]
            for f in range(FRB):
                term = jnp.where(target == f, 1.0, 0.0).astype(jnp.float32) * value
                placed[f] = term if placed[f] is None else placed[f] + term
        for f in range(FRB):
            at = (v, slice(f * width, (f + 1) * width), slice(h * half, (h + 1) * half))
            result[at] = (front[at].astype(jnp.float32) - placed[f]).astype(jnp.bfloat16)
        out_copy(p).start()

    parts = 4
    send_own(0)
    send_l(0)
    for copy in maps:
        copy.wait()
    for v in range(LEVELS):
        rows_of[gz, v] = jnp.full(rows_of.shape[2:], rowmap[0, 0, v], jnp.int32)
    for p in range(phases):
        if p == 0:
            def body(t, _):
                forward(0, t)
                return 0
            lax.fori_loop(1, 3, body, 0)
            for v in range(1, LEVELS):
                send_l(v)
            for g in peers:
                rows_copy(g).start()
            lax.fori_loop(3, last, body, 0)
        elif p < phases - 1:
            for t in range(1, last):
                forward(p, t)
                if t == 1:
                    wait_last(p - 1)
                    if p == 1:
                        wait_l(0)
                if t <= parts:
                    products(p - 1, t - 1, parts)
                if t == parts:
                    exchange(p - 1)
                if t == 3 and p >= 2:
                    finish(p - 2)
        else:
            for t in range(1, last):
                forward(p, t)
                if t == 1:
                    wait_last(p - 1)
                if t <= 2:
                    products(p - 1, 2 * t - 2, parts)
                    products(p - 1, 2 * t - 1, parts)
                if t == 2:
                    exchange(p - 1)
                    acc[p % 2] = product(p, row, 1)
                if t == 3:
                    finish(p - 2)
                if t >= 3:
                    for d in ((1, 2, 3) if t == 3 else (t,)):
                        acc[p % 2] += product(p, lax.rem(row + d, n_row), 1)
                        acc[p % 2] += product(p, lax.rem(row + n_row - d, n_row), 1)
        if p < phases - 1:
            send_own(p + 1)
        if p == 0:
            fronts.wait()
            wait_rows()
        forward_last(p)
        if p == 1:
            wait_l(1)
    p = phases - 1
    finish(p - 1)
    acc[p % 2] += product(p, lax.rem(row + last, n_row), 1)
    acc[p % 2] += product(p, lax.rem(row + n_row - last, n_row), 1)
    wait_last(p)
    acc[p % 2] += product(p, lax.rem(row + last + 1, n_row), 1)
    exchange(p)
    finish(p)

    for way in range(2):
        for q in range(phases):
            at = u_all.at[q, pl.ds(0, depth * last + depth // 2)]
            pltpu.make_async_copy(at, at, zsend.at[way, q]).wait()
    at = l_all.at[pl.ds(0, LEVELS), pl.ds(0, (n_col - 1) * lblocks)]
    pltpu.make_async_copy(at, at, lsend).wait()
    at = rows_of.at[pl.ds(0, n_gz - 1)]
    pltpu.make_async_copy(at, at, rsend).wait()
    for q in range(phases):
        at = sums.at[q, pl.ds(0, n_gz - 1)]
        pltpu.make_async_copy(at, at, asend.at[q]).wait()
    for q in range(phases):
        out_copy(q).wait()


def on_device(lpanel, upanel, rowmap, colmap, blockmask, front_blocks):
    n_row, n_gz, n_col = lax.axis_size("row"), lax.axis_size("gz"), lax.axis_size("col")
    depth = upanel.shape[2]
    width = lpanel.shape[2]
    half = width // HALVES
    phases = LEVELS * HALVES
    lblocks = lpanel.shape[3] // depth
    hops = n_row // 2
    anywhere = pl.BlockSpec(memory_space=pltpu.HBM)
    dma = pltpu.SemaphoreType.DMA
    return pl.pallas_call(
        functools.partial(kernel, n_row, n_gz, n_col),
        out_shape=jax.ShapeDtypeStruct(front_blocks.shape, jnp.bfloat16),
        in_specs=[anywhere] * 6,
        out_specs=anywhere,
        scratch_shapes=[
            pltpu.VMEM((phases, n_row * depth, CB * half), jnp.bfloat16),
            pltpu.VMEM((LEVELS, n_row, width, depth), jnp.bfloat16),
            pltpu.VMEM((2, width, CB * half), jnp.float32),
            pltpu.VMEM((phases, n_gz, width, half), jnp.bfloat16),
            pltpu.VMEM((phases, n_gz, width, half), jnp.bfloat16),
            pltpu.VMEM((n_gz, LEVELS, 8, 128), jnp.int32),
            pltpu.VMEM(front_blocks.shape, jnp.bfloat16),
            pltpu.VMEM(front_blocks.shape, jnp.bfloat16),
            pltpu.SMEM((1, 1, LEVELS), jnp.int32),
            pltpu.SMEM(colmap.shape, jnp.int32),
            pltpu.SMEM(blockmask.shape, jnp.int32),
            dma((2, phases)),
            dma((2, phases, hops, SUBS)),
            dma,
            dma((LEVELS, n_col)),
            dma((phases,)),
            dma((phases, n_gz)),
            dma,
            dma((n_gz,)),
            dma((phases, CB)),
            dma((LEVELS, lblocks)),
            dma,
            dma((phases,)),
            dma((3,)),
        ],
        compiler_params=pltpu.CompilerParams(
            collective_id=0, has_side_effects=True, vmem_limit_bytes=67043328
        ),
    )(lpanel, upanel, jnp.transpose(rowmap, (1, 2, 0)), colmap, blockmask, front_blocks)


def solution(mesh):
    return jax.shard_map(
        on_device,
        mesh=mesh,
        in_specs=(
            P(None, "gz", "row", "col"),
            P(None, "gz", "row", "col"),
            P(None, "gz", "row"),
            P(None, "gz", "col"),
            P(None, "gz", "row", "col"),
            P(None, "row", ("gz", "col")),
        ),
        out_specs=P(None, "row", ("gz", "col")),
        check_vma=False,
    )
```

```python
import functools

import jax
import jax.numpy as jnp
from jax import lax
from jax.experimental import pallas as pl
from jax.experimental.pallas import tpu as pltpu
from jax.sharding import PartitionSpec as P

MESH = pl.DeviceIdType.MESH
CB = 4
FRB = 2
LEVELS = 2
HALVES = 2
SUBS = 4


def kernel(
    n_row, n_gz, n_col,
    l_hbm, u_hbm, rowmap_hbm, colmap_hbm, mask_hbm, front_hbm,
    out_ref,
    u_all, l_all, acc, sums, arrived, rows_of, front,
    rowmap, colmap, mask,
    zsend, zrecv, lsend, lrecv, asend, arecv, rsend, rrecv, usem, lsem, fsem, isem,
):
    row, gz, col = lax.axis_index("row"), lax.axis_index("gz"), lax.axis_index("col")
    phases = LEVELS * HALVES
    depth = u_hbm.shape[2]
    width = l_hbm.shape[2]
    half = width // HALVES
    lblocks = l_hbm.shape[3] // depth
    last = n_row // 2 - 1
    piece = depth // SUBS
    ring = [lax.rem(row + 1, n_row), lax.rem(row + n_row - 1, n_row)]

    def others(me, n):
        return [lax.rem(me + i, n) for i in range(1, n)]

    cores = 2
    chips = n_gz // cores
    chip, core = lax.div(gz, cores), lax.rem(gz, cores)
    order = sorted(range(1, chips), key=lambda d: -min(d, chips - d)) + [0]
    peers = []
    for d in order:
        for k in range(cores):
            if (d, k) != (0, 0):
                peers.append(lax.rem(chip + d, chips) * cores + lax.rem(core + k, cores))

    def own_u(p, j):
        v, h = divmod(p, HALVES)
        return pltpu.make_async_copy(
            u_hbm.at[v, 0, :, pl.ds(j * width + h * half, half)],
            u_all.at[p, pl.ds(row * depth, depth), pl.ds(j * half, half)],
            usem.at[p, j],
        )

    def own_l(v, i):
        return pltpu.make_async_copy(
            l_hbm.at[v, 0, :, pl.ds(i * depth, depth)], l_all.at[v, col * lblocks + i], lsem.at[v, i]
        )

    fronts = pltpu.make_async_copy(front_hbm, front, fsem)
    maps = [
        pltpu.make_async_copy(rowmap_hbm, rowmap, isem.at[0]),
        pltpu.make_async_copy(colmap_hbm, colmap, isem.at[1]),
        pltpu.make_async_copy(mask_hbm, mask, isem.at[2]),
    ]
    for j in range(CB):
        own_u(0, j).start()
    for i in range(lblocks):
        own_l(0, i).start()
    for p in range(1, phases):
        for j in range(CB):
            own_u(p, j).start()
    for v in range(1, LEVELS):
        for i in range(lblocks):
            own_l(v, i).start()
    fronts.start()
    for copy in maps:
        copy.start()

    barrier = pltpu.get_barrier_semaphore()
    for r in ring:
        pl.semaphore_signal(barrier, inc=1, device_id={"row": r}, device_id_type=MESH)
    for c in others(col, n_col):
        pl.semaphore_signal(barrier, inc=1, device_id={"col": c}, device_id_type=MESH)
    for g in peers:
        pl.semaphore_signal(barrier, inc=1, device_id={"gz": g}, device_id_type=MESH)
    pl.semaphore_wait(barrier, 2 + (n_col - 1) + (n_gz - 1))

    def hop(way, p, t, s):
        shard = lax.rem(row + n_row - t, n_row) if way == 0 else lax.rem(row + t, n_row)
        at = u_all.at[p, pl.ds(pl.multiple_of(shard * depth + s * piece, piece), piece)]
        return pltpu.make_async_remote_copy(
            src_ref=at, dst_ref=at, send_sem=zsend.at[way, p], recv_sem=zrecv.at[way, p, t, s],
            device_id={"row": ring[way]}, device_id_type=MESH,
        )

    def arrival(way, p, t, s):
        at = u_all.at[p, pl.ds(0, piece)]
        return pltpu.make_async_copy(at, at, zrecv.at[way, p, t, s])

    longer = (range(SUBS // 2), range(SUBS // 2, SUBS))

    def send_own(p):
        for j in range(CB):
            own_u(p, j).wait()
        for s in range(SUBS):
            for way in range(2):
                hop(way, p, 0, (s + way * SUBS // 2) % SUBS).start()

    def forward(p, t):
        for s in range(SUBS):
            for way in range(2):
                which = (s + way * SUBS // 2) % SUBS
                arrival(way, p, t - 1, which).wait()
                hop(way, p, t, which).start()

    def forward_last(p):
        for s in range(SUBS):
            for way in range(2):
                which = (s + way * SUBS // 2) % SUBS
                arrival(way, p, last - 1, which).wait()
                if which in longer[way]:
                    hop(way, p, last, which).start()

    def wait_last(p):
        for way in range(2):
            for s in longer[way]:
                arrival(way, p, last, s).wait()

    def l_copy(v, c):
        at = l_all.at[v, pl.ds(col * lblocks, lblocks)]
        return pltpu.make_async_remote_copy(
            src_ref=at, dst_ref=at, send_sem=lsend, recv_sem=lrecv.at[v, col],
            device_id={"col": c}, device_id_type=MESH,
        )

    def send_l(v):
        for i in range(lblocks):
            own_l(v, i).wait()
        for c in others(col, n_col):
            l_copy(v, c).start()

    def wait_l(v):
        at = l_all.at[v, pl.ds(0, lblocks)]
        for c in others(col, n_col):
            pltpu.make_async_copy(at, at, lrecv.at[v, c]).wait()

    def rows_copy(g):
        at = rows_of.at[gz]
        return pltpu.make_async_remote_copy(
            src_ref=at, dst_ref=at, send_sem=rsend, recv_sem=rrecv.at[gz],
            device_id={"gz": g}, device_id_type=MESH,
        )

    def wait_rows():
        at = rows_of.at[0]
        for g in peers:
            pltpu.make_async_copy(at, at, rrecv.at[g]).wait()

    def product(p, first, count):
        v = p // HALVES
        left = jnp.concatenate([l_all[v, first + i] for i in range(count)], axis=1) if count > 1 else l_all[v, first]
        right = u_all[p, pl.ds(pl.multiple_of(first * depth, depth), count * depth), :]
        return jnp.dot(left, right, preferred_element_type=jnp.float32)

    def products(p, q, parts):
        size = n_row // parts
        value = product(p, q * size, size)
        if q == 0:
            acc[p] = value
        else:
            acc[p] += value

    def block_copy(p, g):
        return pltpu.make_async_remote_copy(
            src_ref=sums.at[p, g], dst_ref=arrived.at[p, gz], send_sem=asend.at[p], recv_sem=arecv.at[p, gz],
            device_id={"gz": g}, device_id_type=MESH,
        )

    def layer_sum(p, g):
        v = p // HALVES
        total = None
        for j in range(CB):
            keep = jnp.where(colmap[v, 0, j] == g, mask[v, 0, 0, j], 0).astype(jnp.float32)
            term = acc[p, :, j * half : (j + 1) * half] * keep
            total = term if total is None else total + term
        return total.astype(jnp.bfloat16)

    def exchange(p):
        before = None
        for g in peers:
            sums[p, g] = layer_sum(p, g)
            if before is not None:
                block_copy(p, before).start()
            before = g
        arrived[p, gz] = layer_sum(p, gz)
        block_copy(p, before).start()

    def finish(p):
        v, h = divmod(p, HALVES)
        block = arrived.at[p, 0]
        for g in peers:
            pltpu.make_async_copy(block, block, arecv.at[p, g]).wait()
        placed = [None] * FRB
        for g in range(n_gz):
            value = arrived[p, g].astype(jnp.float32)
            target = rows_of[g, v][:1]
            for f in range(FRB):
                term = jnp.where(target == f, 1.0, 0.0).astype(jnp.float32) * value
                placed[f] = term if placed[f] is None else placed[f] + term
        for f in range(FRB):
            at = (v, slice(f * width, (f + 1) * width), slice(h * half, (h + 1) * half))
            out_ref[at] = (front[at].astype(jnp.float32) - placed[f]).astype(jnp.bfloat16)

    def start_products(p):
        acc[p] = product(p, row, 1)

    def pair(p, t):
        acc[p] += product(p, lax.rem(row + t, n_row), 1)
        acc[p] += product(p, lax.rem(row + n_row - t, n_row), 1)

    def farthest(p):
        wait_last(p)
        acc[p] += product(p, lax.rem(row + last + 1, n_row), 1)

    parts = 4

    def whole(p):
        wait_last(p)
        for q in range(parts):
            products(p, q, parts)

    send_own(0)
    send_own(1)
    send_l(0)
    for copy in maps:
        copy.wait()
    for v in range(LEVELS):
        rows_of[gz, v] = jnp.full(rows_of.shape[2:], rowmap[0, 0, v], jnp.int32)

    starts = (0, 0, last - 2, last + 1)
    for r in range(1, starts[-1] + last + 1):
        for p in range(phases):
            t = r - starts[p]
            if t == 0:
                send_own(p)
            elif 0 < t < last:
                forward(p, t)
            elif t == last:
                forward_last(p)
        if r == 3:
            for g in peers:
                rows_copy(g).start()
        if r == 4:
            for v in range(1, LEVELS):
                send_l(v)
        if r == last + 1:
            wait_l(0)
            whole(0)
            exchange(0)
        if r == last + 2:
            whole(1)
            exchange(1)
        if r == last + 3:
            fronts.wait()
            wait_rows()
            for v in range(1, LEVELS):
                wait_l(v)
            finish(0)
        if r == last + 4:
            finish(1)
        for p in range(2, phases):
            t = r - starts[p]
            if r == last + 3:
                if t >= 0:
                    start_products(p)
                for d in range(1, t + 1):
                    pair(p, d)
            elif r > last + 3:
                if 1 <= t <= last:
                    pair(p, t)
                elif t == last + 1:
                    farthest(p)
                    exchange(p)
    p = phases - 1
    farthest(p)
    exchange(p)
    finish(p - 1)
    finish(p)

    for way in range(2):
        for q in range(phases):
            at = u_all.at[q, pl.ds(0, depth * last + depth // 2)]
            pltpu.make_async_copy(at, at, zsend.at[way, q]).wait()
    at = l_all.at[pl.ds(0, LEVELS), pl.ds(0, (n_col - 1) * lblocks)]
    pltpu.make_async_copy(at, at, lsend).wait()
    at = rows_of.at[pl.ds(0, n_gz - 1)]
    pltpu.make_async_copy(at, at, rsend).wait()
    for q in range(phases):
        at = sums.at[q, pl.ds(0, n_gz - 1)]
        pltpu.make_async_copy(at, at, asend.at[q]).wait()


def on_device(lpanel, upanel, rowmap, colmap, blockmask, front_blocks):
    n_row, n_gz, n_col = lax.axis_size("row"), lax.axis_size("gz"), lax.axis_size("col")
    depth = upanel.shape[2]
    width = lpanel.shape[2]
    half = width // HALVES
    phases = LEVELS * HALVES
    lblocks = lpanel.shape[3] // depth
    hops = n_row // 2
    anywhere = pl.BlockSpec(memory_space=pltpu.HBM)
    dma = pltpu.SemaphoreType.DMA
    return pl.pallas_call(
        functools.partial(kernel, n_row, n_gz, n_col),
        out_shape=jax.ShapeDtypeStruct(front_blocks.shape, jnp.bfloat16),
        in_specs=[anywhere] * 6,
        out_specs=pl.BlockSpec(memory_space=pltpu.VMEM),
        scratch_shapes=[
            pltpu.VMEM((phases, n_row * depth, CB * half), jnp.bfloat16),
            pltpu.VMEM((LEVELS, n_row, width, depth), jnp.bfloat16),
            pltpu.VMEM((phases, width, CB * half), jnp.float32),
            pltpu.VMEM((phases, n_gz, width, half), jnp.bfloat16),
            pltpu.VMEM((phases, n_gz, width, half), jnp.bfloat16),
            pltpu.VMEM((n_gz, LEVELS, 8, 128), jnp.int32),
            pltpu.VMEM(front_blocks.shape, jnp.bfloat16),
            pltpu.SMEM((1, 1, LEVELS), jnp.int32),
            pltpu.SMEM(colmap.shape, jnp.int32),
            pltpu.SMEM(blockmask.shape, jnp.int32),
            dma((2, phases)),
            dma((2, phases, hops, SUBS)),
            dma,
            dma((LEVELS, n_col)),
            dma((phases,)),
            dma((phases, n_gz)),
            dma,
            dma((n_gz,)),
            dma((phases, CB)),
            dma((LEVELS, lblocks)),
            dma,
            dma((3,)),
        ],
        compiler_params=pltpu.CompilerParams(
            collective_id=0, has_side_effects=True, vmem_limit_bytes=40 * 1024 * 1024
        ),
    )(
        *(
            pltpu.with_memory_space_constraint(value, pltpu.HBM)
            for value in (lpanel, upanel, jnp.transpose(rowmap, (1, 2, 0)), colmap, blockmask, front_blocks)
        )
    )


def solution(mesh):
    return jax.shard_map(
        on_device,
        mesh=mesh,
        in_specs=(
            P(None, "gz", "row", "col"),
            P(None, "gz", "row", "col"),
            P(None, "gz", "row"),
            P(None, "gz", "col"),
            P(None, "gz", "row", "col"),
            P(None, "row", ("gz", "col")),
        ),
        out_specs=P(None, "row", ("gz", "col")),
        check_vma=False,
    )
```

```python
import functools

import jax
import jax.numpy as jnp
from jax import lax
from jax.experimental import pallas as pl
from jax.experimental.pallas import tpu as pltpu
from jax.sharding import PartitionSpec as P

MESH = pl.DeviceIdType.MESH
CB = 4
FRB = 2
LEVELS = 2
HALVES = 2
SUBS = (2, 2, 4, 4)
SLOTS = 3


def kernel(
    n_row, n_gz, n_col,
    l_hbm, u_hbm, rowmap_hbm, colmap_hbm, mask_hbm, front_hbm,
    out_ref,
    u_all, l_all, acc, sums, arrived, rows_of, front,
    rowmap, colmap, mask,
    zsend, zrecv, lsend, lrecv, asend, arecv, rsend, rrecv, usem, lsem, fsem, isem,
):
    row, gz, col = lax.axis_index("row"), lax.axis_index("gz"), lax.axis_index("col")
    phases = LEVELS * HALVES
    depth = u_hbm.shape[2]
    width = l_hbm.shape[2]
    half = width // HALVES
    lblocks = l_hbm.shape[3] // depth
    last = n_row // 2 - 1
    ring = [lax.rem(row + 1, n_row), lax.rem(row + n_row - 1, n_row)]

    def others(me, n):
        return [lax.rem(me + i, n) for i in range(1, n)]

    cores = 2
    chips = n_gz // cores
    chip, core = lax.div(gz, cores), lax.rem(gz, cores)
    order = sorted(range(1, chips), key=lambda d: -min(d, chips - d)) + [0]
    peers = []
    for d in order:
        for k in range(cores):
            if (d, k) != (0, 0):
                peers.append(lax.rem(chip + d, chips) * cores + lax.rem(core + k, cores))

    barrier = pltpu.get_barrier_semaphore()
    for r in ring:
        pl.semaphore_signal(barrier, inc=1, device_id={"row": r}, device_id_type=MESH)
    for c in others(col, n_col):
        pl.semaphore_signal(barrier, inc=1, device_id={"col": c}, device_id_type=MESH)
    for g in peers:
        pl.semaphore_signal(barrier, inc=1, device_id={"gz": g}, device_id_type=MESH)

    def own_u(p, j):
        v, h = divmod(p, HALVES)
        return pltpu.make_async_copy(
            u_hbm.at[v, 0, :, pl.ds(j * width + h * half, half)],
            u_all.at[p, pl.ds(row * depth, depth), pl.ds(j * half, half)],
            usem.at[p],
        )

    def own_l(v, i):
        return pltpu.make_async_copy(
            l_hbm.at[v, 0, :, pl.ds(i * depth, depth)], l_all.at[v, col * lblocks + i], lsem.at[v]
        )

    fronts = pltpu.make_async_copy(front_hbm, front, fsem)
    maps = [
        pltpu.make_async_copy(rowmap_hbm, rowmap, isem.at[0]),
        pltpu.make_async_copy(colmap_hbm, colmap, isem.at[1]),
        pltpu.make_async_copy(mask_hbm, mask, isem.at[2]),
    ]
    for j in range(CB):
        own_u(0, j).start()
    for i in range(lblocks):
        own_l(0, i).start()
    for p in range(1, phases):
        for j in range(CB):
            own_u(p, j).start()
    for v in range(1, LEVELS):
        for i in range(lblocks):
            own_l(v, i).start()
    fronts.start()
    for copy in maps:
        copy.start()

    pl.semaphore_wait(barrier, 2 + (n_col - 1) + (n_gz - 1))

    def landed(way, p, t, s):
        return zrecv.at[way, SLOTS * sum(SUBS[:p]) + (t % SLOTS) * SUBS[p] + s]

    def hop(way, p, t, s):
        shard = lax.rem(row + n_row - t, n_row) if way == 0 else lax.rem(row + t, n_row)
        piece = depth // SUBS[p]
        at = u_all.at[p, pl.ds(pl.multiple_of(shard * depth + s * piece, piece), piece)]
        return pltpu.make_async_remote_copy(
            src_ref=at, dst_ref=at, send_sem=zsend, recv_sem=landed(way, p, t, s),
            device_id={"row": ring[way]}, device_id_type=MESH,
        )

    def arrival(way, p, t, s):
        at = u_all.at[p, pl.ds(0, depth // SUBS[p])]
        return pltpu.make_async_copy(at, at, landed(way, p, t, s))

    def longer(way, p):
        return range(SUBS[p] // 2) if way == 0 else range(SUBS[p] // 2, SUBS[p])

    def each(p):
        return [(way, (s + way * SUBS[p] // 2) % SUBS[p]) for s in range(SUBS[p]) for way in range(2)]

    def send_own(p):
        at = u_all.at[p, pl.ds(0, depth)]
        pltpu.make_async_copy(at, at, usem.at[p]).wait()
        for way, k in each(p):
            hop(way, p, 0, k).start()

    def forward(p, t):
        for way, k in each(p):
            arrival(way, p, t - 1, k).wait()
            if t < last or k in longer(way, p):
                hop(way, p, t, k).start()

    def wait_last(p):
        for way in range(2):
            for k in longer(way, p):
                arrival(way, p, last, k).wait()

    def l_copy(v, c):
        at = l_all.at[v, pl.ds(col * lblocks, lblocks)]
        return pltpu.make_async_remote_copy(
            src_ref=at, dst_ref=at, send_sem=lsend, recv_sem=lrecv.at[v],
            device_id={"col": c}, device_id_type=MESH,
        )

    def send_l(v):
        at = l_all.at[v, pl.ds(0, lblocks)]
        pltpu.make_async_copy(at, at, lsem.at[v]).wait()
        for c in others(col, n_col):
            l_copy(v, c).start()

    def wait_l(v):
        at = l_all.at[v, pl.ds(0, (n_col - 1) * lblocks)]
        pltpu.make_async_copy(at, at, lrecv.at[v]).wait()

    def rows_copy(g):
        at = rows_of.at[gz]
        return pltpu.make_async_remote_copy(
            src_ref=at, dst_ref=at, send_sem=rsend, recv_sem=rrecv,
            device_id={"gz": g}, device_id_type=MESH,
        )

    def wait_rows():
        at = rows_of.at[pl.ds(0, n_gz - 1)]
        pltpu.make_async_copy(at, at, rrecv).wait()

    def product(p, first, count):
        v = p // HALVES
        left = jnp.concatenate([l_all[v, first + i] for i in range(count)], axis=1) if count > 1 else l_all[v, first]
        right = u_all[p, pl.ds(pl.multiple_of(first * depth, depth), count * depth), :]
        return jnp.dot(left, right, preferred_element_type=jnp.float32)

    def products(p, q, parts):
        size = n_row // parts
        value = product(p, q * size, size)
        if q == 0:
            acc[p] = value
        else:
            acc[p] += value

    def block_copy(p, g):
        return pltpu.make_async_remote_copy(
            src_ref=sums.at[p, g], dst_ref=arrived.at[p, gz], send_sem=asend, recv_sem=arecv.at[p],
            device_id={"gz": g}, device_id_type=MESH,
        )

    def layer_sum(p, g):
        v = p // HALVES
        total = None
        for j in range(CB):
            keep = jnp.where(colmap[v, 0, j] == g, mask[v, 0, 0, j], 0).astype(jnp.float32)
            term = acc[p, :, j * half : (j + 1) * half] * keep
            total = term if total is None else total + term
        return total.astype(jnp.bfloat16)

    def exchange(p):
        before = None
        for g in peers:
            sums[p, g] = layer_sum(p, g)
            if before is not None:
                block_copy(p, before).start()
            before = g
        arrived[p, gz] = layer_sum(p, gz)
        block_copy(p, before).start()

    def finish(p):
        v, h = divmod(p, HALVES)
        block = arrived.at[p, pl.ds(0, n_gz - 1)]
        pltpu.make_async_copy(block, block, arecv.at[p]).wait()
        placed = [None] * FRB
        for g in range(n_gz):
            value = arrived[p, g].astype(jnp.float32)
            target = rows_of[g, v][:1]
            for f in range(FRB):
                term = jnp.where(target == f, 1.0, 0.0).astype(jnp.float32) * value
                placed[f] = term if placed[f] is None else placed[f] + term
        for f in range(FRB):
            at = (v, slice(f * width, (f + 1) * width), slice(h * half, (h + 1) * half))
            out_ref[at] = (front[at].astype(jnp.float32) - placed[f]).astype(jnp.bfloat16)

    def start_products(p):
        acc[p] = product(p, row, 1)

    def pair(p, t):
        acc[p] += product(p, lax.rem(row + t, n_row), 1)
        acc[p] += product(p, lax.rem(row + n_row - t, n_row), 1)

    def farthest(p):
        wait_last(p)
        acc[p] += product(p, lax.rem(row + last + 1, n_row), 1)

    parts = 4

    def whole(p):
        wait_last(p)
        for q in range(parts):
            products(p, q, parts)

    send_own(0)
    send_own(1)
    send_l(0)
    for copy in maps:
        copy.wait()
    for v in range(LEVELS):
        rows_of[gz, v] = jnp.full(rows_of.shape[2:], rowmap[0, 0, v], jnp.int32)

    starts = (0, 0, last - 2, last + 1)
    for r in range(1, starts[-1] + last + 1):
        for p in range(phases):
            t = r - starts[p]
            if t == 0:
                send_own(p)
            elif 0 < t <= last:
                forward(p, t)
        if r == 3:
            for g in peers:
                rows_copy(g).start()
        if r == 4:
            for v in range(1, LEVELS):
                send_l(v)
        if r == last + 1:
            wait_l(0)
            whole(0)
            exchange(0)
        if r == last + 2:
            whole(1)
            exchange(1)
        if r == last + 3:
            fronts.wait()
            wait_rows()
            for v in range(1, LEVELS):
                wait_l(v)
            finish(0)
        if r == last + 4:
            finish(1)
        for p in range(2, phases):
            t = r - starts[p]
            if r == last + 3:
                if t >= 0:
                    start_products(p)
                for d in range(1, t + 1):
                    pair(p, d)
            elif r > last + 3:
                if 1 <= t <= last:
                    pair(p, t)
                elif t == last + 1:
                    farthest(p)
                    exchange(p)
    p = phases - 1
    farthest(p)
    exchange(p)
    finish(p - 1)
    finish(p)

    hops = 2 * last + 1
    at = u_all.at[:, pl.ds(0, depth * hops)]
    pltpu.make_async_copy(at, at, zsend).wait()
    at = l_all.at[:, pl.ds(0, (n_col - 1) * lblocks)]
    pltpu.make_async_copy(at, at, lsend).wait()
    at = rows_of.at[pl.ds(0, n_gz - 1)]
    pltpu.make_async_copy(at, at, rsend).wait()
    at = sums.at[:, pl.ds(0, n_gz - 1)]
    pltpu.make_async_copy(at, at, asend).wait()


def on_device(lpanel, upanel, rowmap, colmap, blockmask, front_blocks):
    n_row, n_gz, n_col = lax.axis_size("row"), lax.axis_size("gz"), lax.axis_size("col")
    depth = upanel.shape[2]
    width = lpanel.shape[2]
    half = width // HALVES
    phases = LEVELS * HALVES
    lblocks = lpanel.shape[3] // depth
    anywhere = pl.BlockSpec(memory_space=pltpu.HBM)
    dma = pltpu.SemaphoreType.DMA
    return pl.pallas_call(
        functools.partial(kernel, n_row, n_gz, n_col),
        out_shape=jax.ShapeDtypeStruct(front_blocks.shape, jnp.bfloat16),
        in_specs=[anywhere] * 6,
        out_specs=pl.BlockSpec(memory_space=pltpu.VMEM),
        scratch_shapes=[
            pltpu.VMEM((phases, n_row * depth, CB * half), jnp.bfloat16),
            pltpu.VMEM((LEVELS, n_row, width, depth), jnp.bfloat16),
            pltpu.VMEM((phases, width, CB * half), jnp.float32),
            pltpu.VMEM((phases, n_gz, width, half), jnp.bfloat16),
            pltpu.VMEM((phases, n_gz, width, half), jnp.bfloat16),
            pltpu.VMEM((n_gz, LEVELS, 8, 128), jnp.int32),
            pltpu.VMEM(front_blocks.shape, jnp.bfloat16),
            pltpu.SMEM((1, 1, LEVELS), jnp.int32),
            pltpu.SMEM(colmap.shape, jnp.int32),
            pltpu.SMEM(blockmask.shape, jnp.int32),
            dma,
            dma((2, SLOTS * sum(SUBS))),
            dma,
            dma((LEVELS,)),
            dma,
            dma((phases,)),
            dma,
            dma,
            dma((phases,)),
            dma((LEVELS,)),
            dma,
            dma((3,)),
        ],
        compiler_params=pltpu.CompilerParams(
            collective_id=0, has_side_effects=True, vmem_limit_bytes=40 * 1024 * 1024
        ),
    )(
        *(
            pltpu.with_memory_space_constraint(value, pltpu.HBM)
            for value in (lpanel, upanel, jnp.transpose(rowmap, (1, 2, 0)), colmap, blockmask, front_blocks)
        )
    )


def solution(mesh):
    return jax.shard_map(
        on_device,
        mesh=mesh,
        in_specs=(
            P(None, "gz", "row", "col"),
            P(None, "gz", "row", "col"),
            P(None, "gz", "row"),
            P(None, "gz", "col"),
            P(None, "gz", "row", "col"),
            P(None, "row", ("gz", "col")),
        ),
        out_specs=P(None, "row", ("gz", "col")),
        check_vma=False,
    )
```

```python
import functools

import jax
import jax.numpy as jnp
from jax import lax
from jax.experimental import pallas as pl
from jax.experimental.pallas import tpu as pltpu
from jax.sharding import PartitionSpec as P

MESH = pl.DeviceIdType.MESH
CB = 4
FRB = 2
LEVELS = 2
HALVES = 2
SUBS = (1, 1, 4, 4)
SLOTS = 3
EARLY = 1


def kernel(
    n_row, n_gz, n_col,
    l_hbm, u_hbm, rowmap_hbm, colmap_hbm, mask_hbm, front_hbm,
    out_ref,
    u_all, l_all, acc, sums, arrived, rows_of, front,
    rowmap, colmap, mask,
    zsend, zrecv, lsend, lrecv, asend, arecv, rsend, rrecv, usem, lsem, fsem, isem, vouch,
):
    row, gz, col = lax.axis_index("row"), lax.axis_index("gz"), lax.axis_index("col")
    phases = LEVELS * HALVES
    depth = u_hbm.shape[2]
    width = l_hbm.shape[2]
    half = width // HALVES
    lblocks = l_hbm.shape[3] // depth
    last = n_row // 2 - 1
    ring = [lax.rem(row + 1, n_row), lax.rem(row + n_row - 1, n_row)]

    def others(me, n):
        return [lax.rem(me + i, n) for i in range(1, n)]

    cores = 2
    chips = n_gz // cores
    chip, core = lax.div(gz, cores), lax.rem(gz, cores)
    order = sorted(range(1, chips), key=lambda d: -min(d, chips - d)) + [0]
    peers = []
    for d in order:
        for k in range(cores):
            if (d, k) != (0, 0):
                peers.append(lax.rem(chip + d, chips) * cores + lax.rem(core + k, cores))
    early = [jnp.where(gz == EARLY, peers[0], EARLY)]
    early += [jnp.where(g == EARLY, peers[0], g) for g in peers[1:]]

    barrier = pltpu.get_barrier_semaphore()
    near_gz = [
        lax.rem(chip + d, chips) * cores + lax.rem(core + k, cores)
        for d in (0, 1, chips - 1)
        for k in range(cores)
        if (d, k) != (0, 0)
    ]
    near_col = [lax.rem(col + 1, n_col), lax.rem(col + n_col - 1, n_col)]
    for r in ring:
        pl.semaphore_signal(barrier, inc=1, device_id={"row": r}, device_id_type=MESH)
    for g in near_gz:
        pl.semaphore_signal(barrier, inc=1, device_id={"gz": g}, device_id_type=MESH)
    for c in near_col:
        pl.semaphore_signal(barrier, inc=1, device_id={"col": c}, device_id_type=MESH)

    def own_u(p, j):
        v, h = divmod(p, HALVES)
        return pltpu.make_async_copy(
            u_hbm.at[v, 0, :, pl.ds(j * width + h * half, half)],
            u_all.at[p, pl.ds(row * depth, depth), pl.ds(j * half, half)],
            usem.at[p],
        )

    def own_l(v, i):
        return pltpu.make_async_copy(
            l_hbm.at[v, 0, :, pl.ds(i * depth, depth)], l_all.at[v, col * lblocks + i], lsem.at[v]
        )

    fronts = pltpu.make_async_copy(front_hbm, front, fsem)
    maps = [
        pltpu.make_async_copy(rowmap_hbm, rowmap, isem.at[0]),
        pltpu.make_async_copy(colmap_hbm, colmap, isem.at[1]),
        pltpu.make_async_copy(mask_hbm, mask, isem.at[2]),
    ]
    for p in range(2):
        for j in range(CB):
            own_u(p, j).start()

    pl.semaphore_wait(barrier, len(ring) + len(near_gz) + len(near_col))

    def landed(way, p, t, s):
        return zrecv.at[way, SLOTS * sum(SUBS[:p]) + (t % SLOTS) * SUBS[p] + s]

    def hop(way, p, t, s):
        shard = lax.rem(row + n_row - t, n_row) if way == 0 else lax.rem(row + t, n_row)
        piece = depth // SUBS[p]
        at = u_all.at[p, pl.ds(pl.multiple_of(shard * depth + s * piece, piece), piece)]
        return pltpu.make_async_remote_copy(
            src_ref=at, dst_ref=at, send_sem=zsend, recv_sem=landed(way, p, t, s),
            device_id={"row": ring[way]}, device_id_type=MESH,
        )

    def arrival(way, p, t, s):
        at = u_all.at[p, pl.ds(0, depth // SUBS[p])]
        return pltpu.make_async_copy(at, at, landed(way, p, t, s))

    def longer(way, p):
        if SUBS[p] == 1:
            return range(1) if way == p % 2 else range(0)
        return range(SUBS[p] // 2) if way == 0 else range(SUBS[p] // 2, SUBS[p])

    def each(p):
        return [(way, (s + way * SUBS[p] // 2) % SUBS[p]) for s in range(SUBS[p]) for way in range(2)]

    def send_own(p):
        at = u_all.at[p, pl.ds(0, depth)]
        pltpu.make_async_copy(at, at, usem.at[p]).wait()
        for way, k in each(p):
            hop(way, p, 0, k).start()

    def forward(p, t):
        for way, k in each(p):
            arrival(way, p, t - 1, k).wait()
            if t < last or k in longer(way, p):
                hop(way, p, t, k).start()

    def wait_last(p):
        for way in range(2):
            for k in longer(way, p):
                arrival(way, p, last, k).wait()

    def l_copy(v, c):
        at = l_all.at[v, pl.ds(col * lblocks, lblocks)]
        return pltpu.make_async_remote_copy(
            src_ref=at, dst_ref=at, send_sem=lsend, recv_sem=lrecv.at[v],
            device_id={"col": c}, device_id_type=MESH,
        )

    def send_l(v):
        at = l_all.at[v, pl.ds(0, lblocks)]
        pltpu.make_async_copy(at, at, lsem.at[v]).wait()
        for c in others(col, n_col):
            l_copy(v, c).start()

    def wait_l(v):
        at = l_all.at[v, pl.ds(0, (n_col - 1) * lblocks)]
        pltpu.make_async_copy(at, at, lrecv.at[v]).wait()

    def rows_copy(g):
        at = rows_of.at[gz]
        return pltpu.make_async_remote_copy(
            src_ref=at, dst_ref=at, send_sem=rsend, recv_sem=rrecv,
            device_id={"gz": g}, device_id_type=MESH,
        )

    def wait_rows():
        at = rows_of.at[pl.ds(0, n_gz - 1)]
        pltpu.make_async_copy(at, at, rrecv).wait()

    def product(p, shards):
        v = p // HALVES
        left = [l_all[v, k] for k in shards]
        right = [u_all[p, pl.ds(pl.multiple_of(k * depth, depth), depth), :] for k in shards]
        if len(shards) > 1:
            left, right = [jnp.concatenate(left, axis=1)], [jnp.concatenate(right, axis=0)]
        return jnp.dot(left[0], right[0], preferred_element_type=jnp.float32)

    def block_copy(p, g):
        return pltpu.make_async_remote_copy(
            src_ref=sums.at[p, g], dst_ref=arrived.at[p, gz], send_sem=asend, recv_sem=arecv.at[p],
            device_id={"gz": g}, device_id_type=MESH,
        )

    def layer_sum(p, g):
        v = p // HALVES
        total = None
        for j in range(CB):
            keep = jnp.where(colmap[v, 0, j] == g, mask[v, 0, 0, j], 0).astype(jnp.float32)
            term = acc[p, :, j * half : (j + 1) * half] * keep
            total = term if total is None else total + term
        return total.astype(jnp.bfloat16)

    def exchange(p):
        before = None
        for g in early:
            sums[p, g] = layer_sum(p, g)
            if before is not None:
                block_copy(p, before).start()
            before = g
        arrived[p, gz] = layer_sum(p, gz)
        block_copy(p, before).start()

    def finish(p):
        v, h = divmod(p, HALVES)
        block = arrived.at[p, pl.ds(0, n_gz - 1)]
        pltpu.make_async_copy(block, block, arecv.at[p]).wait()
        placed = [None] * FRB
        for g in range(n_gz):
            value = arrived[p, g].astype(jnp.float32)
            target = rows_of[g, v][:1]
            for f in range(FRB):
                term = jnp.where(target == f, 1.0, 0.0).astype(jnp.float32) * value
                placed[f] = term if placed[f] is None else placed[f] + term
        for f in range(FRB):
            at = (v, slice(f * width, (f + 1) * width), slice(h * half, (h + 1) * half))
            out_ref[at] = (front[at].astype(jnp.float32) - placed[f]).astype(jnp.bfloat16)

    def near(p, t):
        if t == 0:
            acc[p] = product(p, [row])
        else:
            acc[p] += product(p, [lax.rem(row + t, n_row), lax.rem(row + n_row - t, n_row)])

    def farthest(p):
        wait_last(p)
        acc[p] += product(p, [lax.rem(row + last + 1, n_row)])

    send_own(0)
    send_own(1)
    for v in range(LEVELS):
        for i in range(lblocks):
            own_l(v, i).start()
    for copy in maps:
        copy.start()
    for p in range(2, phases):
        for j in range(CB):
            own_u(p, j).start()
    fronts.start()
    pl.semaphore_signal(
        vouch.at[0], inc=1, device_id={"gz": lax.rem(chip + 1, chips) * cores + core}, device_id_type=MESH
    )
    pl.semaphore_signal(vouch.at[1], inc=1, device_id={"col": near_col[0]}, device_id_type=MESH)
    pl.semaphore_wait(vouch.at[1], 1)
    for v in range(LEVELS):
        send_l(v)
    for copy in maps:
        copy.wait()
    for v in range(LEVELS):
        rows_of[gz, v] = jnp.full(rows_of.shape[2:], rowmap[0, 0, v], jnp.int32)

    starts = (0, 0, last - 2, last)
    begin = (3, 4, 0, 0)
    for r in range(1, starts[-1] + last + 1):
        if r == 2:
            pl.semaphore_wait(vouch.at[0], 1)
            for g in peers:
                rows_copy(g).start()
        if r == begin[0]:
            wait_l(0)
        if r == starts[2]:
            for v in range(1, LEVELS):
                wait_l(v)
        if r == starts[2] + last + 1:
            farthest(2)
            exchange(2)
        for p in range(phases):
            t = r - starts[p]
            if t == 0:
                send_own(p)
            elif 0 < t <= last:
                forward(p, t)
            if begin[p] <= t <= last:
                for d in range(0 if t == begin[p] else t, t + 1):
                    near(p, d)
        if r == last + 1:
            farthest(0)
            exchange(0)
        if r == last + 2:
            farthest(1)
            exchange(1)
        if r == last + 3:
            fronts.wait()
            wait_rows()
            finish(0)
        if r == last + 4:
            finish(1)
    p = phases - 1
    farthest(p)
    exchange(p)
    finish(p - 1)
    finish(p)

    hops = 2 * last + 1
    at = u_all.at[:, pl.ds(0, depth * hops)]
    pltpu.make_async_copy(at, at, zsend).wait()
    at = l_all.at[:, pl.ds(0, (n_col - 1) * lblocks)]
    pltpu.make_async_copy(at, at, lsend).wait()
    at = rows_of.at[pl.ds(0, n_gz - 1)]
    pltpu.make_async_copy(at, at, rsend).wait()
    at = sums.at[:, pl.ds(0, n_gz - 1)]
    pltpu.make_async_copy(at, at, asend).wait()


def on_device(lpanel, upanel, rowmap, colmap, blockmask, front_blocks):
    n_row, n_gz, n_col = lax.axis_size("row"), lax.axis_size("gz"), lax.axis_size("col")
    depth = upanel.shape[2]
    width = lpanel.shape[2]
    half = width // HALVES
    phases = LEVELS * HALVES
    lblocks = lpanel.shape[3] // depth
    anywhere = pl.BlockSpec(memory_space=pltpu.HBM)
    dma = pltpu.SemaphoreType.DMA
    return pl.pallas_call(
        functools.partial(kernel, n_row, n_gz, n_col),
        out_shape=jax.ShapeDtypeStruct(front_blocks.shape, jnp.bfloat16),
        in_specs=[anywhere] * 6,
        out_specs=pl.BlockSpec(memory_space=pltpu.VMEM),
        scratch_shapes=[
            pltpu.VMEM((phases, n_row * depth, CB * half), jnp.bfloat16),
            pltpu.VMEM((LEVELS, n_row, width, depth), jnp.bfloat16),
            pltpu.VMEM((phases, width, CB * half), jnp.float32),
            pltpu.VMEM((phases, n_gz, width, half), jnp.bfloat16),
            pltpu.VMEM((phases, n_gz, width, half), jnp.bfloat16),
            pltpu.VMEM((n_gz, LEVELS, 8, 128), jnp.int32),
            pltpu.VMEM(front_blocks.shape, jnp.bfloat16),
            pltpu.SMEM((1, 1, LEVELS), jnp.int32),
            pltpu.SMEM(colmap.shape, jnp.int32),
            pltpu.SMEM(blockmask.shape, jnp.int32),
            dma,
            dma((2, SLOTS * sum(SUBS))),
            dma,
            dma((LEVELS,)),
            dma,
            dma((phases,)),
            dma,
            dma,
            dma((phases,)),
            dma((LEVELS,)),
            dma,
            dma((3,)),
            pltpu.SemaphoreType.REGULAR((2,)),
        ],
        compiler_params=pltpu.CompilerParams(
            collective_id=0, has_side_effects=True, vmem_limit_bytes=40 * 1024 * 1024
        ),
    )(
        *(
            pltpu.with_memory_space_constraint(value, pltpu.HBM)
            for value in (lpanel, upanel, jnp.transpose(rowmap, (1, 2, 0)), colmap, blockmask, front_blocks)
        )
    )


def solution(mesh):
    return jax.shard_map(
        on_device,
        mesh=mesh,
        in_specs=(
            P(None, "gz", "row", "col"),
            P(None, "gz", "row", "col"),
            P(None, "gz", "row"),
            P(None, "gz", "col"),
            P(None, "gz", "row", "col"),
            P(None, "row", ("gz", "col")),
        ),
        out_specs=P(None, "row", ("gz", "col")),
        check_vma=False,
    )
```

```python
import functools

import jax
import jax.numpy as jnp
from jax import lax
from jax.experimental import pallas as pl
from jax.experimental.pallas import tpu as pltpu
from jax.sharding import PartitionSpec as P

MESH = pl.DeviceIdType.MESH
CB = 4
FRB = 2
LEVELS = 2
HALVES = 2
SUBS = (1, 1, 4, 4)
SLOTS = 3
EARLY = 1


def kernel(
    n_row, n_gz, n_col,
    l_hbm, u_hbm, rowmap_hbm, colmap_hbm, mask_hbm, front_hbm,
    out_ref,
    u_all, l_all, acc, sums, arrived, rows_of, front,
    rowmap, colmap, mask,
    zsend, zrecv, lsend, lrecv, asend, arecv, rsend, rrecv, usem, lsem, fsem, isem, vouch,
):
    row, gz, col = lax.axis_index("row"), lax.axis_index("gz"), lax.axis_index("col")
    phases = LEVELS * HALVES
    depth = u_hbm.shape[2]
    width = l_hbm.shape[2]
    half = width // HALVES
    lblocks = l_hbm.shape[3] // depth
    last = n_row // 2 - 1
    ring = [lax.rem(row + 1, n_row), lax.rem(row + n_row - 1, n_row)]

    def others(me, n):
        return [lax.rem(me + i, n) for i in range(1, n)]

    cores = 2
    chips = n_gz // cores
    chip, core = lax.div(gz, cores), lax.rem(gz, cores)
    order = sorted(range(1, chips), key=lambda d: min(d, chips - d)) + [0]
    peers = []
    for d in order:
        for k in range(cores):
            if (d, k) != (0, 0):
                peers.append(lax.rem(chip + d, chips) * cores + lax.rem(core + k, cores))
    early = [jnp.where(gz == EARLY, peers[0], EARLY)]
    early += [jnp.where(g == EARLY, peers[0], g) for g in peers[1:]]

    barrier = pltpu.get_barrier_semaphore()
    near_gz = [
        lax.rem(chip + d, chips) * cores + lax.rem(core + k, cores)
        for d in (0, 1, chips - 1)
        for k in range(cores)
        if (d, k) != (0, 0)
    ]
    near_col = [lax.rem(col + 1, n_col), lax.rem(col + n_col - 1, n_col)]
    for r in ring:
        pl.semaphore_signal(barrier, inc=1, device_id={"row": r}, device_id_type=MESH)
    for g in near_gz:
        pl.semaphore_signal(barrier, inc=1, device_id={"gz": g}, device_id_type=MESH)
    for c in near_col:
        pl.semaphore_signal(barrier, inc=1, device_id={"col": c}, device_id_type=MESH)

    def own_u(p, j):
        v, h = divmod(p, HALVES)
        return pltpu.make_async_copy(
            u_hbm.at[v, 0, :, pl.ds(j * width + h * half, half)],
            u_all.at[p, pl.ds(row * depth, depth), pl.ds(j * half, half)],
            usem.at[p],
        )

    def own_l(v, i):
        return pltpu.make_async_copy(
            l_hbm.at[v, 0, :, pl.ds(i * depth, depth)], l_all.at[v, col * lblocks + i], lsem.at[v]
        )

    fronts = pltpu.make_async_copy(front_hbm, front, fsem)
    maps = [
        pltpu.make_async_copy(rowmap_hbm, rowmap, isem.at[0]),
        pltpu.make_async_copy(colmap_hbm, colmap, isem.at[1]),
        pltpu.make_async_copy(mask_hbm, mask, isem.at[2]),
    ]
    for p in range(2):
        for j in range(CB):
            own_u(p, j).start()

    pl.semaphore_wait(barrier, len(ring) + len(near_gz) + len(near_col))

    def landed(way, p, t, s):
        return zrecv.at[way, SLOTS * sum(SUBS[:p]) + (t % SLOTS) * SUBS[p] + s]

    def hop(way, p, t, s):
        shard = lax.rem(row + n_row - t, n_row) if way == 0 else lax.rem(row + t, n_row)
        piece = depth // SUBS[p]
        at = u_all.at[p, pl.ds(pl.multiple_of(shard * depth + s * piece, piece), piece)]
        return pltpu.make_async_remote_copy(
            src_ref=at, dst_ref=at, send_sem=zsend, recv_sem=landed(way, p, t, s),
            device_id={"row": ring[way]}, device_id_type=MESH,
        )

    def arrival(way, p, t, s):
        at = u_all.at[p, pl.ds(0, depth // SUBS[p])]
        return pltpu.make_async_copy(at, at, landed(way, p, t, s))

    def longer(way, p):
        if SUBS[p] == 1:
            return range(1) if way == p % 2 else range(0)
        return range(SUBS[p] // 2) if way == 0 else range(SUBS[p] // 2, SUBS[p])

    def each(p):
        return [(way, (s + way * SUBS[p] // 2) % SUBS[p]) for s in range(SUBS[p]) for way in range(2)]

    def send_own(p):
        at = u_all.at[p, pl.ds(0, depth)]
        pltpu.make_async_copy(at, at, usem.at[p]).wait()
        for way, k in each(p):
            hop(way, p, 0, k).start()

    def forward(p, t):
        for way, k in each(p):
            arrival(way, p, t - 1, k).wait()
            if t < last or k in longer(way, p):
                hop(way, p, t, k).start()

    def wait_last(p):
        for way in range(2):
            for k in longer(way, p):
                arrival(way, p, last, k).wait()

    def l_copy(v, c):
        at = l_all.at[v, pl.ds(col * lblocks, lblocks)]
        return pltpu.make_async_remote_copy(
            src_ref=at, dst_ref=at, send_sem=lsend, recv_sem=lrecv.at[v],
            device_id={"col": c}, device_id_type=MESH,
        )

    def send_l(v):
        at = l_all.at[v, pl.ds(0, lblocks)]
        pltpu.make_async_copy(at, at, lsem.at[v]).wait()
        for c in others(col, n_col):
            l_copy(v, c).start()

    def wait_l(v):
        at = l_all.at[v, pl.ds(0, (n_col - 1) * lblocks)]
        pltpu.make_async_copy(at, at, lrecv.at[v]).wait()

    def rows_copy(g):
        at = rows_of.at[gz]
        return pltpu.make_async_remote_copy(
            src_ref=at, dst_ref=at, send_sem=rsend, recv_sem=rrecv,
            device_id={"gz": g}, device_id_type=MESH,
        )

    def wait_rows():
        at = rows_of.at[pl.ds(0, n_gz - 1)]
        pltpu.make_async_copy(at, at, rrecv).wait()

    def product(p, shards):
        v = p // HALVES
        left = [l_all[v, k] for k in shards]
        right = [u_all[p, pl.ds(pl.multiple_of(k * depth, depth), depth), :] for k in shards]
        if len(shards) > 1:
            left, right = [jnp.concatenate(left, axis=1)], [jnp.concatenate(right, axis=0)]
        return jnp.dot(left[0], right[0], preferred_element_type=jnp.float32)

    def block_copy(p, g):
        return pltpu.make_async_remote_copy(
            src_ref=sums.at[p, g], dst_ref=arrived.at[p, gz], send_sem=asend, recv_sem=arecv.at[p],
            device_id={"gz": g}, device_id_type=MESH,
        )

    def layer_sum(p, g):
        v = p // HALVES
        total = None
        for j in range(CB):
            keep = jnp.where(colmap[v, 0, j] == g, mask[v, 0, 0, j], 0).astype(jnp.float32)
            term = acc[p, :, j * half : (j + 1) * half] * keep
            total = term if total is None else total + term
        return total.astype(jnp.bfloat16)

    def exchange(p):
        before = None
        for g in early:
            sums[p, g] = layer_sum(p, g)
            if before is not None:
                block_copy(p, before).start()
            before = g
        arrived[p, gz] = layer_sum(p, gz)
        block_copy(p, before).start()

    def finish(p):
        v, h = divmod(p, HALVES)
        block = arrived.at[p, pl.ds(0, n_gz - 1)]
        pltpu.make_async_copy(block, block, arecv.at[p]).wait()
        placed = [None] * FRB
        for g in range(n_gz):
            value = arrived[p, g].astype(jnp.float32)
            target = rows_of[g, v][:1]
            for f in range(FRB):
                term = jnp.where(target == f, 1.0, 0.0).astype(jnp.float32) * value
                placed[f] = term if placed[f] is None else placed[f] + term
        for f in range(FRB):
            at = (v, slice(f * width, (f + 1) * width), slice(h * half, (h + 1) * half))
            out_ref[at] = (front[at].astype(jnp.float32) - placed[f]).astype(jnp.bfloat16)

    def near(p, t):
        if t == 0:
            acc[p] = product(p, [row])
        else:
            acc[p] += product(p, [lax.rem(row + t, n_row), lax.rem(row + n_row - t, n_row)])

    def farthest(p):
        wait_last(p)
        acc[p] += product(p, [lax.rem(row + last + 1, n_row)])

    send_own(0)
    send_own(1)
    for v in range(LEVELS):
        for i in range(lblocks):
            own_l(v, i).start()
    for copy in maps:
        copy.start()
    for p in range(2, phases):
        for j in range(CB):
            own_u(p, j).start()
    fronts.start()
    pl.semaphore_signal(
        vouch.at[0], inc=1, device_id={"gz": lax.rem(chip + 1, chips) * cores + core}, device_id_type=MESH
    )
    pl.semaphore_signal(vouch.at[1], inc=1, device_id={"col": near_col[0]}, device_id_type=MESH)
    pl.semaphore_wait(vouch.at[1], 1)
    for v in range(LEVELS):
        send_l(v)
    for copy in maps:
        copy.wait()
    for v in range(LEVELS):
        rows_of[gz, v] = jnp.full(rows_of.shape[2:], rowmap[0, 0, v], jnp.int32)

    starts = (0, 0, last - 2, last)
    begin = (3, 4, 0, 0)
    for r in range(1, starts[-1] + last + 1):
        if r == 2:
            pl.semaphore_wait(vouch.at[0], 1)
            for g in peers:
                rows_copy(g).start()
        if r == begin[0]:
            wait_l(0)
        if r == starts[2]:
            for v in range(1, LEVELS):
                wait_l(v)
        if r == starts[2] + last + 1:
            farthest(2)
            exchange(2)
        for p in range(phases):
            t = r - starts[p]
            if t == 0:
                send_own(p)
            elif 0 < t <= last:
                forward(p, t)
            if begin[p] <= t <= last:
                for d in range(0 if t == begin[p] else t, t + 1):
                    near(p, d)
        if r == last + 1:
            farthest(0)
            exchange(0)
        if r == last + 2:
            farthest(1)
            exchange(1)
        if r == last + 3:
            fronts.wait()
            wait_rows()
            finish(0)
        if r == last + 4:
            finish(1)
    p = phases - 1
    farthest(p)
    exchange(p)
    finish(p - 1)
    finish(p)

    hops = 2 * last + 1
    at = u_all.at[:, pl.ds(0, depth * hops)]
    pltpu.make_async_copy(at, at, zsend).wait()
    at = l_all.at[:, pl.ds(0, (n_col - 1) * lblocks)]
    pltpu.make_async_copy(at, at, lsend).wait()
    at = rows_of.at[pl.ds(0, n_gz - 1)]
    pltpu.make_async_copy(at, at, rsend).wait()
    at = sums.at[:, pl.ds(0, n_gz - 1)]
    pltpu.make_async_copy(at, at, asend).wait()


def on_device(lpanel, upanel, rowmap, colmap, blockmask, front_blocks):
    n_row, n_gz, n_col = lax.axis_size("row"), lax.axis_size("gz"), lax.axis_size("col")
    depth = upanel.shape[2]
    width = lpanel.shape[2]
    half = width // HALVES
    phases = LEVELS * HALVES
    lblocks = lpanel.shape[3] // depth
    anywhere = pl.BlockSpec(memory_space=pltpu.HBM)
    dma = pltpu.SemaphoreType.DMA
    return pl.pallas_call(
        functools.partial(kernel, n_row, n_gz, n_col),
        out_shape=jax.ShapeDtypeStruct(front_blocks.shape, jnp.bfloat16),
        in_specs=[anywhere] * 6,
        out_specs=pl.BlockSpec(memory_space=pltpu.VMEM),
        scratch_shapes=[
            pltpu.VMEM((phases, n_row * depth, CB * half), jnp.bfloat16),
            pltpu.VMEM((LEVELS, n_row, width, depth), jnp.bfloat16),
            pltpu.VMEM((phases, width, CB * half), jnp.float32),
            pltpu.VMEM((phases, n_gz, width, half), jnp.bfloat16),
            pltpu.VMEM((phases, n_gz, width, half), jnp.bfloat16),
            pltpu.VMEM((n_gz, LEVELS, 8, 128), jnp.int32),
            pltpu.VMEM(front_blocks.shape, jnp.bfloat16),
            pltpu.SMEM((1, 1, LEVELS), jnp.int32),
            pltpu.SMEM(colmap.shape, jnp.int32),
            pltpu.SMEM(blockmask.shape, jnp.int32),
            dma,
            dma((2, SLOTS * sum(SUBS))),
            dma,
            dma((LEVELS,)),
            dma,
            dma((phases,)),
            dma,
            dma,
            dma((phases,)),
            dma((LEVELS,)),
            dma,
            dma((3,)),
            pltpu.SemaphoreType.REGULAR((2,)),
        ],
        compiler_params=pltpu.CompilerParams(
            collective_id=0, has_side_effects=True, vmem_limit_bytes=40 * 1024 * 1024
        ),
    )(
        *(
            pltpu.with_memory_space_constraint(value, pltpu.HBM)
            for value in (lpanel, upanel, jnp.transpose(rowmap, (1, 2, 0)), colmap, blockmask, front_blocks)
        )
    )


def solution(mesh):
    return jax.shard_map(
        on_device,
        mesh=mesh,
        in_specs=(
            P(None, "gz", "row", "col"),
            P(None, "gz", "row", "col"),
            P(None, "gz", "row"),
            P(None, "gz", "col"),
            P(None, "gz", "row", "col"),
            P(None, "row", ("gz", "col")),
        ),
        out_specs=P(None, "row", ("gz", "col")),
        check_vma=False,
    )
```

```python
import functools

import jax
import jax.numpy as jnp
from jax import lax
from jax.experimental import pallas as pl
from jax.experimental.pallas import tpu as pltpu
from jax.sharding import PartitionSpec as P

MESH = pl.DeviceIdType.MESH
CB = 4
FRB = 2
LEVELS = 2
HALVES = 2
SUBS = (1, 1, 4, 4)
SLOTS = 3
EARLY = 1


def kernel(
    n_row, n_gz, n_col,
    l_hbm, u_hbm, rowmap_hbm, colmap_hbm, mask_hbm, front_hbm,
    out_ref,
    u_all, l_all, acc, sums, arrived, rows_of, front,
    rowmap, colmap, mask,
    zsend, zrecv, lsend, lrecv, asend, arecv, rsend, rrecv, usem, lsem, fsem, isem, vouch,
):
    row, gz, col = lax.axis_index("row"), lax.axis_index("gz"), lax.axis_index("col")
    phases = LEVELS * HALVES
    depth = u_hbm.shape[2]
    width = l_hbm.shape[2]
    half = width // HALVES
    lblocks = l_hbm.shape[3] // depth
    last = n_row // 2 - 1
    ring = [lax.rem(row + 1, n_row), lax.rem(row + n_row - 1, n_row)]

    def others(me, n):
        return [lax.rem(me + i, n) for i in range(1, n)]

    cores = 2
    chips = n_gz // cores
    chip, core = lax.div(gz, cores), lax.rem(gz, cores)
    order = sorted(range(1, chips), key=lambda d: min(d, chips - d)) + [0]
    peers = []
    for d in order:
        for k in range(cores):
            if (d, k) != (0, 0):
                peers.append(lax.rem(chip + d, chips) * cores + lax.rem(core + k, cores))
    early = [jnp.where(gz == EARLY, peers[0], EARLY)]
    early += [jnp.where(g == EARLY, peers[0], g) for g in peers[1:]]

    barrier = pltpu.get_barrier_semaphore()
    near_gz = [
        lax.rem(chip + d, chips) * cores + lax.rem(core + k, cores)
        for d in (0, 1, chips - 1)
        for k in range(cores)
        if (d, k) != (0, 0)
    ]
    near_col = [lax.rem(col + 1, n_col), lax.rem(col + n_col - 1, n_col)]
    for r in ring:
        pl.semaphore_signal(barrier, inc=1, device_id={"row": r}, device_id_type=MESH)
    for g in near_gz:
        pl.semaphore_signal(barrier, inc=1, device_id={"gz": g}, device_id_type=MESH)
    for c in near_col:
        pl.semaphore_signal(barrier, inc=1, device_id={"col": c}, device_id_type=MESH)

    def own_u(p, j):
        v, h = divmod(p, HALVES)
        return pltpu.make_async_copy(
            u_hbm.at[v, 0, :, pl.ds(j * width + h * half, half)],
            u_all.at[p, pl.ds(row * depth, depth), pl.ds(j * half, half)],
            usem.at[p],
        )

    def own_l(v, i):
        return pltpu.make_async_copy(
            l_hbm.at[v, 0, :, pl.ds(i * depth, depth)], l_all.at[v, col * lblocks + i], lsem.at[v]
        )

    fronts = pltpu.make_async_copy(front_hbm, front, fsem)
    maps = [
        pltpu.make_async_copy(rowmap_hbm, rowmap, isem.at[0]),
        pltpu.make_async_copy(colmap_hbm, colmap, isem.at[1]),
        pltpu.make_async_copy(mask_hbm, mask, isem.at[2]),
    ]
    for p in range(2):
        for j in range(CB):
            own_u(p, j).start()

    pl.semaphore_wait(barrier, len(ring) + len(near_gz) + len(near_col))

    def landed(way, p, t, s):
        return zrecv.at[way, SLOTS * sum(SUBS[:p]) + (t % SLOTS) * SUBS[p] + s]

    def hop(way, p, t, s):
        shard = lax.rem(row + n_row - t, n_row) if way == 0 else lax.rem(row + t, n_row)
        piece = depth // SUBS[p]
        at = u_all.at[p, pl.ds(pl.multiple_of(shard * depth + s * piece, piece), piece)]
        return pltpu.make_async_remote_copy(
            src_ref=at, dst_ref=at, send_sem=zsend, recv_sem=landed(way, p, t, s),
            device_id={"row": ring[way]}, device_id_type=MESH,
        )

    def arrival(way, p, t, s):
        at = u_all.at[p, pl.ds(0, depth // SUBS[p])]
        return pltpu.make_async_copy(at, at, landed(way, p, t, s))

    def longer(way, p):
        if SUBS[p] == 1:
            return range(1) if way == p % 2 else range(0)
        return range(SUBS[p] // 2) if way == 0 else range(SUBS[p] // 2, SUBS[p])

    def each(p):
        return [(way, (s + way * SUBS[p] // 2) % SUBS[p]) for s in range(SUBS[p]) for way in range(2)]

    def send_own(p):
        at = u_all.at[p, pl.ds(0, depth)]
        pltpu.make_async_copy(at, at, usem.at[p]).wait()
        for way, k in each(p):
            hop(way, p, 0, k).start()

    def forward(p, t):
        for way, k in each(p):
            arrival(way, p, t - 1, k).wait()
            if t < last or k in longer(way, p):
                hop(way, p, t, k).start()

    def wait_last(p):
        for way in range(2):
            for k in longer(way, p):
                arrival(way, p, last, k).wait()

    def l_copy(v, c):
        at = l_all.at[v, pl.ds(col * lblocks, lblocks)]
        return pltpu.make_async_remote_copy(
            src_ref=at, dst_ref=at, send_sem=lsend, recv_sem=lrecv.at[v],
            device_id={"col": c}, device_id_type=MESH,
        )

    def send_l(v):
        at = l_all.at[v, pl.ds(0, lblocks)]
        pltpu.make_async_copy(at, at, lsem.at[v]).wait()
        for c in others(col, n_col):
            l_copy(v, c).start()

    def wait_l(v):
        at = l_all.at[v, pl.ds(0, (n_col - 1) * lblocks)]
        pltpu.make_async_copy(at, at, lrecv.at[v]).wait()

    def rows_copy(g):
        at = rows_of.at[gz]
        return pltpu.make_async_remote_copy(
            src_ref=at, dst_ref=at, send_sem=rsend, recv_sem=rrecv,
            device_id={"gz": g}, device_id_type=MESH,
        )

    def wait_rows():
        at = rows_of.at[pl.ds(0, n_gz - 1)]
        pltpu.make_async_copy(at, at, rrecv).wait()

    def product(p, shards):
        v = p // HALVES
        left = [l_all[v, k] for k in shards]
        right = [u_all[p, pl.ds(pl.multiple_of(k * depth, depth), depth), :] for k in shards]
        if len(shards) > 1:
            left, right = [jnp.concatenate(left, axis=1)], [jnp.concatenate(right, axis=0)]
        return jnp.dot(left[0], right[0], preferred_element_type=jnp.float32)

    def block_copy(p, g):
        return pltpu.make_async_remote_copy(
            src_ref=sums.at[p, g], dst_ref=arrived.at[p, gz], send_sem=asend, recv_sem=arecv.at[p + gz if p == phases - 1 else p],
            device_id={"gz": g}, device_id_type=MESH,
        )

    def layer_sum(p, g):
        v = p // HALVES
        total = None
        for j in range(CB):
            keep = jnp.where(colmap[v, 0, j] == g, mask[v, 0, 0, j], 0).astype(jnp.float32)
            term = acc[p, :, j * half : (j + 1) * half] * keep
            total = term if total is None else total + term
        return total.astype(jnp.bfloat16)

    def exchange(p):
        before = None
        for g in early:
            sums[p, g] = layer_sum(p, g)
            if before is not None:
                block_copy(p, before).start()
            before = g
        arrived[p, gz] = layer_sum(p, gz)
        block_copy(p, before).start()

    def finish(p):
        v, h = divmod(p, HALVES)
        final = p == phases - 1
        if not final:
            block = arrived.at[p, pl.ds(0, n_gz - 1)]
            pltpu.make_async_copy(block, block, arecv.at[p]).wait()
        placed = [None] * FRB
        for g in [gz, peers[-1], *peers[:-1]] if final else range(n_gz):
            if final and g is not gz:
                block = arrived.at[p, 0]
                pltpu.make_async_copy(block, block, arecv.at[p + g]).wait()
            value = arrived[p, g].astype(jnp.float32)
            target = rows_of[g, v][:1]
            for f in range(FRB):
                term = jnp.where(target == f, 1.0, 0.0).astype(jnp.float32) * value
                placed[f] = term if placed[f] is None else placed[f] + term
        for f in range(FRB):
            at = (v, slice(f * width, (f + 1) * width), slice(h * half, (h + 1) * half))
            out_ref[at] = (front[at].astype(jnp.float32) - placed[f]).astype(jnp.bfloat16)

    def near(p, t):
        if t == 0:
            acc[p] = product(p, [row])
        else:
            acc[p] += product(p, [lax.rem(row + t, n_row), lax.rem(row + n_row - t, n_row)])

    def farthest(p):
        wait_last(p)
        acc[p] += product(p, [lax.rem(row + last + 1, n_row)])

    send_own(0)
    send_own(1)
    for v in range(LEVELS):
        for i in range(lblocks):
            own_l(v, i).start()
    for copy in maps:
        copy.start()
    for p in range(2, phases):
        for j in range(CB):
            own_u(p, j).start()
    fronts.start()
    pl.semaphore_signal(
        vouch.at[0], inc=1, device_id={"gz": lax.rem(chip + 1, chips) * cores + core}, device_id_type=MESH
    )
    pl.semaphore_signal(vouch.at[1], inc=1, device_id={"col": near_col[0]}, device_id_type=MESH)
    pl.semaphore_wait(vouch.at[1], 1)
    for v in range(LEVELS):
        send_l(v)
    for copy in maps:
        copy.wait()
    for v in range(LEVELS):
        rows_of[gz, v] = jnp.full(rows_of.shape[2:], rowmap[0, 0, v], jnp.int32)

    starts = (0, 0, last - 2, last)
    begin = (3, 4, 0, 0)
    for r in range(1, starts[-1] + last + 1):
        if r == 2:
            pl.semaphore_wait(vouch.at[0], 1)
            for g in peers:
                rows_copy(g).start()
        if r == begin[0]:
            wait_l(0)
        if r == starts[2]:
            for v in range(1, LEVELS):
                wait_l(v)
        if r == starts[2] + last + 1:
            farthest(2)
            exchange(2)
        for p in range(phases):
            t = r - starts[p]
            if t == 0:
                send_own(p)
            elif 0 < t <= last:
                forward(p, t)
            if begin[p] <= t <= last:
                for d in range(0 if t == begin[p] else t, t + 1):
                    near(p, d)
        if r == last + 1:
            farthest(0)
            exchange(0)
        if r == last + 2:
            farthest(1)
            exchange(1)
        if r == last + 3:
            fronts.wait()
            wait_rows()
            finish(0)
        if r == last + 4:
            finish(1)
    p = phases - 1
    farthest(p)
    exchange(p)
    finish(p - 1)
    finish(p)

    hops = 2 * last + 1
    at = u_all.at[:, pl.ds(0, depth * hops)]
    pltpu.make_async_copy(at, at, zsend).wait()
    at = l_all.at[:, pl.ds(0, (n_col - 1) * lblocks)]
    pltpu.make_async_copy(at, at, lsend).wait()
    at = rows_of.at[pl.ds(0, n_gz - 1)]
    pltpu.make_async_copy(at, at, rsend).wait()
    at = sums.at[:, pl.ds(0, n_gz - 1)]
    pltpu.make_async_copy(at, at, asend).wait()


def on_device(lpanel, upanel, rowmap, colmap, blockmask, front_blocks):
    n_row, n_gz, n_col = lax.axis_size("row"), lax.axis_size("gz"), lax.axis_size("col")
    depth = upanel.shape[2]
    width = lpanel.shape[2]
    half = width // HALVES
    phases = LEVELS * HALVES
    lblocks = lpanel.shape[3] // depth
    anywhere = pl.BlockSpec(memory_space=pltpu.HBM)
    dma = pltpu.SemaphoreType.DMA
    return pl.pallas_call(
        functools.partial(kernel, n_row, n_gz, n_col),
        out_shape=jax.ShapeDtypeStruct(front_blocks.shape, jnp.bfloat16),
        in_specs=[anywhere] * 6,
        out_specs=pl.BlockSpec(memory_space=pltpu.VMEM),
        scratch_shapes=[
            pltpu.VMEM((phases, n_row * depth, CB * half), jnp.bfloat16),
            pltpu.VMEM((LEVELS, n_row, width, depth), jnp.bfloat16),
            pltpu.VMEM((phases, width, CB * half), jnp.float32),
            pltpu.VMEM((phases, n_gz, width, half), jnp.bfloat16),
            pltpu.VMEM((phases, n_gz, width, half), jnp.bfloat16),
            pltpu.VMEM((n_gz, LEVELS, 8, 128), jnp.int32),
            pltpu.VMEM(front_blocks.shape, jnp.bfloat16),
            pltpu.SMEM((1, 1, LEVELS), jnp.int32),
            pltpu.SMEM(colmap.shape, jnp.int32),
            pltpu.SMEM(blockmask.shape, jnp.int32),
            dma,
            dma((2, SLOTS * sum(SUBS))),
            dma,
            dma((LEVELS,)),
            dma,
            dma((phases - 1 + n_gz,)),
            dma,
            dma,
            dma((phases,)),
            dma((LEVELS,)),
            dma,
            dma((3,)),
            pltpu.SemaphoreType.REGULAR((2,)),
        ],
        compiler_params=pltpu.CompilerParams(
            collective_id=0, has_side_effects=True, vmem_limit_bytes=40 * 1024 * 1024
        ),
    )(
        *(
            pltpu.with_memory_space_constraint(value, pltpu.HBM)
            for value in (lpanel, upanel, jnp.transpose(rowmap, (1, 2, 0)), colmap, blockmask, front_blocks)
        )
    )


def solution(mesh):
    return jax.shard_map(
        on_device,
        mesh=mesh,
        in_specs=(
            P(None, "gz", "row", "col"),
            P(None, "gz", "row", "col"),
            P(None, "gz", "row"),
            P(None, "gz", "col"),
            P(None, "gz", "row", "col"),
            P(None, "row", ("gz", "col")),
        ),
        out_specs=P(None, "row", ("gz", "col")),
        check_vma=False,
    )
```
